32 devices in a mesh: role: 2 (over core), ctx: 2 (over y), req: 8 (over z, x).
Axes of the slice: x: 2, y: 2, z: 4, core: 2. Of those that a mesh axis runs over, the one named last changes fastest.
Arguments:
- cache: bfloat16 [16, 8192, 576], P(None, ('ctx', 'req'), 'role'), may hold values from -8 to 8
- lengths: int32 [16], replicated, may hold values from 2 to 8192
- request_decode_slot: int32 [16], replicated, may hold values from 0 to 15, as said below
- q_nope: bfloat16 [16, 4, 16384], P('req', None, ('role', 'ctx')), may hold values from -6 to 6
- q_rope: bfloat16 [16, 4, 8192], P('req', None, ('role', 'ctx')), may hold values from -8 to 8
- new_latent: bfloat16 [16, 4, 576], P('req'), may hold values from -4.1875 to 4.1875
- w_key: bfloat16 [128, 128, 512], P(('role', 'ctx')), may hold values from -0.5 to 0.5
- value_up_weight: bfloat16 [128, 512, 128], P(('role', 'ctx')), may hold values from -1 to 1
Outputs:
- attended: bfloat16 [16, 4, 16384], P('req', None, ('role', 'ctx'))
The draws below stay inside these ranges and needn't reach their ends.
Inputs may be any that keep to these rules, and one draw needn't show every extreme that they name: A permutation of the slots; request r is owned by req index request_decode_slot[r] // 2.
All inputs are finite; a program needn't handle non-finite values.
Results may differ from the reference program's by a relative error of at most 0.007.
Values may be sent and summed in bfloat16 or wider, within the bound.
A program may use at most 128 MiB of HBM per device.

```python
import jax
import jax.numpy as jnp
from jax import lax

HEADS = 128
NOPE = 128
ROPE = 64
LATENT = 512
VDIM = 128
REQ_DEV = 2
BLOCK = 4096
STEPS = 4
REQS = 16
MAXLEN = 8192
N_CTX = 2
N_REQ = 8


def owner_table(key):
    return jax.random.permutation(jax.random.fold_in(key, 101), REQS).astype(jnp.int32)


def draw_request_decode_slot(key, part):
    return owner_table(key)


def draw_cache(key, part):
    base = jax.random.fold_in(key, 303)

    def one_request(index):
        first, second = jax.random.split(jax.random.fold_in(base, index))
        latent = jnp.clip(jax.random.normal(first, (MAXLEN, LATENT), jnp.float32) * 0.5, -3.0, 3.0)
        rotary = jnp.clip(jax.random.normal(second, (MAXLEN, ROPE), jnp.float32), -6.0, 6.0)
        return jnp.concatenate([latent, rotary], axis=1).astype(jnp.bfloat16)
    values = lax.map(one_request, jnp.arange(REQS, dtype=jnp.int32))
    return values


def draw_q_rope(key, part):
    values = jax.random.normal(jax.random.fold_in(key, 404), (REQS, STEPS, HEADS * ROPE), jnp.float32)
    values = jnp.clip(values, -6.0, 6.0)
    return values.astype(jnp.bfloat16)


def plant(drawn, stream_key, least, top_value):
    longest = drawn.shape.index(max(drawn.shape))
    spots = []
    for shift in (0, 1):
        where = [jax.random.randint(jax.random.fold_in(stream_key, axis), (), 0, length) for axis, length in enumerate(drawn.shape)]
        where[longest] = (where[longest] + shift) % drawn.shape[longest]
        spots.append(tuple(where))
    return drawn.at[spots[0]].set(least).at[spots[1]].set(top_value)


def shard_levels(key, dims, shards, least, largest):
    level = 1.0
    for position, shards_of in shards:
        draws = jax.random.uniform(jax.random.fold_in(jax.random.fold_in(key, 6), position), (shards_of,), jnp.float32, least / len(shards), largest / len(shards))
        level = level * jnp.repeat(jnp.exp(draws), dims[position] // shards_of).reshape((-1,) + (1,) * (len(dims) - 1 - position))
    return level


def noise(own_key, shape, deviation, reach, pieces=(), kind=jnp.bfloat16):
    gain = shard_levels(own_key, shape, pieces, -0.22, 0.18) if pieces else 1.0
    values = jax.random.normal(own_key, shape, jnp.float32) * deviation * gain
    return jnp.minimum(jnp.maximum(values, -reach), reach).astype(kind)


def setup_inputs(seed: int = 0) -> dict:
    key_of = jax.random.split(jax.random.key(seed), 9)
    return {
        "cache": draw_cache(jax.random.fold_in(key_of[8], 71), 0),
        "lengths": plant(jax.random.randint(key_of[1], (REQS,), 2, MAXLEN + 1), jax.random.fold_in(key_of[1], 1), 2, MAXLEN).astype(jnp.int32),
        "request_decode_slot": draw_request_decode_slot(jax.random.fold_in(key_of[8], 71), 0),
        "q_nope": noise(key_of[3], (REQS, STEPS, HEADS * NOPE), 1.0, 6.0, ((0, 8), (2, 4))),
        "q_rope": draw_q_rope(jax.random.fold_in(key_of[8], 71), 0),
        "new_latent": noise(key_of[5], (REQS, STEPS, LATENT + ROPE), 0.7, 4.1875, ((0, 8),)),
        "w_key": noise(key_of[6], (HEADS, NOPE, LATENT), NOPE ** -0.5, 0.5, ((0, 4),)),
        "value_up_weight": noise(key_of[7], (HEADS, LATENT, VDIM), (LATENT // 16) ** -0.5, 1.0, ((0, 4),)),
    }


def reference(cache, lengths, request_decode_slot, q_nope, q_rope, new_latent, w_key, value_up_weight):
    total_reqs = request_decode_slot.shape[0]
    inverse = jnp.zeros((total_reqs,), jnp.int32).at[request_decode_slot].set(jnp.arange(total_reqs, dtype=jnp.int32))
    softmax_scale = (NOPE + ROPE) ** -0.5
    key_weights = w_key.astype(jnp.float32)
    value_matrices = value_up_weight.astype(jnp.float32)
    step_ids = jnp.arange(STEPS, dtype=jnp.int32)
    causal = (step_ids[None, :] <= step_ids[:, None])[None, :, None, :]
    positions = jnp.arange(MAXLEN, dtype=jnp.int32)

    def one_owner(owner):
        first = (owner * REQ_DEV).astype(jnp.int32)
        requests = lax.dynamic_slice_in_dim(inverse, first, REQ_DEV)
        payload = cache[requests].astype(jnp.float32)
        visible = (positions[None, :] < lengths[requests][:, None])[:, None, None, :]
        queries = lax.dynamic_slice_in_dim(q_nope, first, REQ_DEV).astype(jnp.float32)
        queries = queries.reshape(REQ_DEV, STEPS, HEADS, NOPE)
        absorbed = jnp.einsum("gshd,hdk->gshk", queries, key_weights).astype(jnp.bfloat16)
        absorbed = lax.optimization_barrier(absorbed).astype(jnp.float32)
        rotary = lax.dynamic_slice_in_dim(q_rope, first, REQ_DEV).astype(jnp.float32)
        rotary = rotary.reshape(REQ_DEV, STEPS, HEADS, ROPE)
        query_rows = jnp.concatenate([absorbed, rotary], axis=3)
        fresh_rows = lax.dynamic_slice_in_dim(new_latent, first, REQ_DEV).astype(jnp.float32)
        scores = jnp.einsum("gshk,gpk->gshp", query_rows, payload) * softmax_scale
        fresh_scores = jnp.einsum("gshk,gtk->gsht", query_rows, fresh_rows) * softmax_scale
        highest = jnp.maximum(jnp.max(jnp.where(visible, scores, -1e30), axis=3),
                              jnp.max(jnp.where(causal, fresh_scores, -1e30), axis=3))
        weights = jnp.where(visible, jnp.exp(scores - highest[..., None]), 0.0)
        fresh_weights = jnp.where(causal, jnp.exp(fresh_scores - highest[..., None]), 0.0)
        normalizer = jnp.sum(weights, axis=3) + jnp.sum(fresh_weights, axis=3)
        rounded = lax.optimization_barrier(weights.astype(jnp.bfloat16)).astype(jnp.float32)
        rounded = rounded.reshape(REQ_DEV, STEPS, HEADS, N_CTX, BLOCK)
        fresh_rounded = lax.optimization_barrier(fresh_weights.astype(jnp.bfloat16)).astype(jnp.float32)
        latent_rows = payload[:, :, :LATENT].reshape(REQ_DEV, N_CTX, BLOCK, LATENT)
        partials = jnp.einsum("gshcp,gcpk->gshck", rounded, latent_rows)
        fresh_part = jnp.einsum("gsht,gtk->gshk", fresh_rounded, fresh_rows[:, :, :LATENT])
        partials = partials.at[:, :, :, 0].add(fresh_part)
        partials = lax.optimization_barrier(partials.astype(jnp.bfloat16)).astype(jnp.float32)
        numerators = jnp.sum(partials, axis=3)
        combined_result = (numerators / normalizer[..., None]).astype(jnp.bfloat16)
        combined_result = lax.optimization_barrier(combined_result).astype(jnp.float32)
        output_rows = jnp.einsum("jnay,ayp->jnap", combined_result, value_matrices).astype(jnp.bfloat16)
        return output_rows.reshape(REQ_DEV, STEPS, HEADS * VDIM)

    stacked = lax.map(one_owner, jnp.arange(N_REQ, dtype=jnp.int32))
    return stacked.reshape(total_reqs, STEPS, HEADS * VDIM)
```

```python
import functools

import jax
import jax.numpy as jnp
from jax import lax
from jax.experimental import pallas as pl
from jax.experimental.pallas import tpu as pltpu
from jax.sharding import PartitionSpec as P


NEG = -1e30


def flash_kernel(scale, steps, latent, info, q_ref, own_a, own_b, far_a, far_b, new_ref, out_ref, lse_ref, keys):
    i = pl.program_id(0)
    role, own_base, far_base, fresh_on = info[0], info[1], info[2], info[3]
    visible = info[4 + i]
    n_ctx, _, rows, width = q_ref.shape
    half, span = own_a.shape[1], own_a.shape[2]
    here = pl.ds(pl.multiple_of(role * half, half), half)
    there = pl.ds(pl.multiple_of((1 - role) * half, half), half)
    keys[here, :span] = own_a[0]
    keys[there, :span] = own_b[0]
    keys[here, span:] = far_a[0]
    keys[there, span:] = far_b[0]
    total = n_ctx * rows
    q = q_ref[...].reshape(total, width)
    k = keys[...]
    scores = lax.dot_general(q, k, (((1,), (0,)), ((), ())), preferred_element_type=jnp.float32) * scale
    column = lax.broadcasted_iota(jnp.int32, (1, 2 * span), 1)
    position = jnp.where(column < span, own_base + column, far_base + column - span)
    seen = position < visible
    new = new_ref[0]
    fresh = lax.dot_general(q, new, (((1,), (1,)), ((), ())), preferred_element_type=jnp.float32) * scale
    token = lax.broadcasted_iota(jnp.int32, fresh.shape, 1)
    step = lax.rem(lax.broadcasted_iota(jnp.int32, fresh.shape, 0) // (rows // steps), steps)
    causal = jnp.logical_and(token <= step, fresh_on > 0)
    scores = jnp.where(seen, scores, NEG)
    fresh = jnp.where(causal, fresh, NEG)
    top = jnp.maximum(jnp.max(scores, axis=1, keepdims=True), jnp.max(fresh, axis=1, keepdims=True))
    weights = jnp.where(seen, jnp.exp(scores - top), 0.0)
    fresh_weights = jnp.where(causal, jnp.exp(fresh - top), 0.0)
    norm = jnp.sum(weights, axis=1, keepdims=True) + jnp.sum(fresh_weights, axis=1, keepdims=True)
    acc = lax.dot_general(
        weights.astype(jnp.bfloat16), k[:latent], (((1,), (1,)), ((), ())), preferred_element_type=jnp.float32
    )
    acc += jnp.dot(fresh_weights.astype(jnp.bfloat16), new[:, :latent], preferred_element_type=jnp.float32)
    live = norm > 0.0
    safe = jnp.where(live, norm, 1.0)
    out = (acc / safe).astype(jnp.bfloat16)
    out_ref[...] = out.reshape(out_ref.shape)
    lse = jnp.where(live, top + jnp.log(safe), NEG)
    flat = jnp.transpose(jnp.broadcast_to(lse, (total, 128)))[0:1, :]
    for c in range(n_ctx):
        lse_ref[c, 0] = flat[:, c * rows:(c + 1) * rows]


def flash(info, queries, own_a, own_b, far_a, far_b, new, scale, steps, latent):
    n_ctx, count, rows, width = queries.shape
    half, span = own_a.shape[1:]
    piece = pl.BlockSpec((1, half, span), lambda i, s: (i, 0, 0))
    flops = 4 * count * n_ctx * rows * width * 2 * span
    grid_spec = pltpu.PrefetchScalarGridSpec(
        num_scalar_prefetch=1,
        grid=(count,),
        in_specs=[
            pl.BlockSpec((n_ctx, 1, rows, width), lambda i, s: (0, i, 0, 0)),
            piece, piece, piece, piece,
            pl.BlockSpec((1,) + new.shape[1:], lambda i, s: (lax.rem(i, new.shape[0]), 0, 0)),
        ],
        out_specs=[
            pl.BlockSpec((n_ctx, 1, rows, latent), lambda i, s: (0, i, 0, 0)),
            pl.BlockSpec((n_ctx, 1, 1, rows), lambda i, s: (0, i, 0, 0)),
        ],
        scratch_shapes=[pltpu.VMEM((2 * half, 2 * span), jnp.bfloat16)],
    )
    return pl.pallas_call(
        functools.partial(flash_kernel, scale, steps, latent),
        grid_spec=grid_spec,
        out_shape=[
            jax.ShapeDtypeStruct((n_ctx, count, rows, latent), jnp.bfloat16),
            jax.ShapeDtypeStruct((n_ctx, count, 1, rows), jnp.float32),
        ],
        compiler_params=pltpu.CompilerParams(vmem_limit_bytes=32 * 1024 * 1024),
        cost_estimate=pl.CostEstimate(flops=flops, bytes_accessed=count * 4 * half * span * 2, transcendentals=0),
    )(info, queries, own_a, own_b, far_a, far_b, new)


def shards(cache, lengths, request_decode_slot, q_nope, q_rope, new_latent, w_key, value_up_weight):
    total_reqs = request_decode_slot.shape[0]
    n_req = lax.axis_size("req")
    n_ctx = lax.axis_size("ctx")
    req_dev = total_reqs // n_req
    me = lax.axis_index("req")
    ctx = lax.axis_index("ctx")
    role = lax.axis_index("role")
    groups = n_req // 2
    group, side = me // 2, me % 2
    heads, nope, latent = w_key.shape
    steps = q_nope.shape[1]
    rope = q_rope.shape[2] // heads
    span = cache.shape[1]
    scale = (nope + rope) ** (-0.5)

    swap = [(i, i ^ 1) for i in range(n_req)]
    other = [(0, 1), (1, 0)]

    def hop(k):
        return [(i, ((i // 2 - k) % groups) * 2 + i % 2) for i in range(n_req)]

    def turn(k):
        return [(i, (i + k) % n_ctx) for i in range(n_ctx)]

    slots = jnp.arange(total_reqs, dtype=jnp.int32)
    inverse = jnp.sum(
        jnp.where(request_decode_slot[None, :] == slots[:, None], slots[None, :], 0), axis=1
    ).astype(jnp.int32)
    order = (group + jnp.arange(groups, dtype=jnp.int32)) % groups

    raw = jnp.concatenate([q_nope, q_rope], axis=2)
    raws = [raw] + [lax.ppermute(raw, "req", hop(k)) for k in range(1, groups)]

    def rows_of(which):
        index = (order[:, None] * 2 + which) * req_dev + jnp.arange(req_dev, dtype=jnp.int32)[None, :]
        return inverse[index]

    mine, theirs = rows_of(side), rows_of(1 - side)
    turned = jnp.swapaxes(cache, 1, 2)
    far_a = [lax.ppermute(turned[theirs[k]], "req", swap) for k in range(groups)]
    own_a = [turned[mine[k]] for k in range(groups)]
    own_b = [lax.ppermute(x, "role", other) for x in own_a]
    far_b = [lax.ppermute(x, "role", other) for x in far_a]

    raws = jnp.stack(raws).reshape(groups * req_dev, steps, -1)
    count = groups * req_dev
    split = heads * nope
    absorbed = jnp.einsum(
        "bshd,hdk->bshk",
        raws[:, :, :split].reshape(count, steps, heads, nope),
        w_key,
        preferred_element_type=jnp.float32,
    ).astype(jnp.bfloat16)
    queries = jnp.concatenate(
        [absorbed, raws[:, :, split:].reshape(count, steps, heads, rope)], axis=3
    ).reshape(count, steps * heads, latent + rope)
    queries = [queries] + [lax.ppermute(queries, "ctx", turn(k)) for k in range(1, n_ctx)]
    queries = jnp.stack(queries)

    new = jnp.pad(new_latent, ((0, 0), (0, 128 - steps), (0, 0)))
    base = ctx * n_req * span
    merged, lses = [], []
    for k in range(groups):
        fresh_on = ((ctx == 0) & (k == 0)).astype(jnp.int32)
        info = jnp.concatenate(
            [jnp.stack([role, base + me * span, base + (me ^ 1) * span, fresh_on]), lengths[mine[k]]]
        ).astype(jnp.int32)
        part = queries[:, k * req_dev:(k + 1) * req_dev]
        out, lse = flash(info, part, own_a[k], own_b[k], far_a[k], far_b[k], new, scale, steps, latent)
        outs = [out[0]] + [lax.ppermute(out[j], "ctx", turn(n_ctx - j)) for j in range(1, n_ctx)]
        lsel = [lse[0]] + [lax.ppermute(lse[j], "ctx", turn(n_ctx - j)) for j in range(1, n_ctx)]
        lsel = jnp.stack(lsel)[:, :, 0, :]
        top = jnp.max(lsel, axis=0)
        share = jnp.exp(lsel - top[None])
        norm = jnp.sum(share, axis=0)
        share = share / norm[None]
        merged.append(sum(o.astype(jnp.float32) * share[j][..., None] for j, o in enumerate(outs)).astype(jnp.bfloat16))
        lses.append(top + jnp.log(norm))
    merged = jnp.concatenate(merged).reshape(count, steps, heads, latent)
    vdim = value_up_weight.shape[2]
    attended = jnp.einsum(
        "poay,ayx->poax", merged, value_up_weight, preferred_element_type=jnp.float32
    ).astype(jnp.bfloat16).reshape(groups, req_dev, steps, heads * vdim)
    back_o, back_l = [attended[0]], [lses[0]]
    for k in range(1, groups):
        back_o.append(lax.ppermute(attended[k], "req", hop(groups - k)))
        back_l.append(lax.ppermute(lses[k], "req", hop(groups - k)))
    back_l = jnp.stack(back_l)
    top = jnp.max(back_l, axis=0)
    share = jnp.exp(back_l - top[None])
    share = (share / jnp.sum(share, axis=0)[None]).reshape(groups, req_dev, steps, heads)
    result = 0.0
    for k in range(groups):
        piece = back_o[k].reshape(req_dev, steps, heads, vdim).astype(jnp.float32)
        result = result + piece * share[k][..., None]
    return result.astype(jnp.bfloat16).reshape(req_dev, steps, heads * vdim)


def solution(mesh):
    placed = (
        P(None, ("ctx", "req"), "role"),
        P(),
        P(),
        P("req", None, ("role", "ctx")),
        P("req", None, ("role", "ctx")),
        P("req", None, None),
        P(("role", "ctx"), None, None),
        P(("role", "ctx"), None, None),
    )
    return jax.shard_map(
        shards,
        mesh=mesh,
        in_specs=placed,
        out_specs=P("req", None, ("role", "ctx")),
        check_vma=False,
    )
```

```python
import functools

import jax
import jax.numpy as jnp
from jax import lax
from jax.experimental import pallas as pl
from jax.experimental.pallas import tpu as pltpu
from jax.sharding import PartitionSpec as P


NEG = -1e30


def pack_kernel(index, src_ref, dst_ref):
    dst_ref[...] = src_ref[...]


def pack(rows, index):
    count = index.shape[0]
    tail = rows.shape[1:]
    return pl.pallas_call(
        pack_kernel,
        grid_spec=pltpu.PrefetchScalarGridSpec(
            num_scalar_prefetch=1,
            grid=(count,),
            in_specs=[pl.BlockSpec((1,) + tail, lambda i, s: (s[i], 0, 0))],
            out_specs=pl.BlockSpec((1,) + tail, lambda i, s: (i, 0, 0)),
        ),
        out_shape=jax.ShapeDtypeStruct((count,) + tail, rows.dtype),
        cost_estimate=pl.CostEstimate(flops=0, bytes_accessed=4 * count * tail[0] * tail[1], transcendentals=0),
    )(index, rows)


def flash_kernel(scale, steps, latent, n_ctx, info, *refs):
    q_refs, refs = refs[:n_ctx], refs[n_ctx:]
    own_a, own_b, far_a, far_b, new_ref = refs[:5]
    out_refs, lse_refs, keys = refs[5:5 + n_ctx], refs[5 + n_ctx:5 + 2 * n_ctx], refs[-1]
    i = pl.program_id(0)
    role, own_base, far_base, fresh_on = info[0], info[1], info[2], info[3]
    visible = info[4 + i]
    _, rows, width = q_refs[0].shape
    half, span = own_a.shape[1], own_a.shape[2]
    here = pl.ds(pl.multiple_of(role * half, half), half)
    there = pl.ds(pl.multiple_of((1 - role) * half, half), half)
    keys[here, :span] = own_a[0]
    keys[there, :span] = own_b[0]
    keys[here, span:] = far_a[0]
    keys[there, span:] = far_b[0]
    k = keys[...]
    column = lax.broadcasted_iota(jnp.int32, (1, 2 * span), 1)
    position = jnp.where(column < span, own_base + column, far_base + column - span)
    seen = position < visible
    new = new_ref[0]
    for c in range(n_ctx):
        q = q_refs[c][0]
        scores = lax.dot_general(q, k, (((1,), (0,)), ((), ())), preferred_element_type=jnp.float32) * scale
        fresh = lax.dot_general(q, new, (((1,), (1,)), ((), ())), preferred_element_type=jnp.float32) * scale
        token = lax.broadcasted_iota(jnp.int32, fresh.shape, 1)
        step = lax.broadcasted_iota(jnp.int32, fresh.shape, 0) // (rows // steps)
        causal = jnp.logical_and(token <= step, fresh_on > 0)
        scores = jnp.where(seen, scores, NEG)
        fresh = jnp.where(causal, fresh, NEG)
        top = jnp.maximum(jnp.max(scores, axis=1, keepdims=True), jnp.max(fresh, axis=1, keepdims=True))
        weights = jnp.where(seen, jnp.exp(scores - top), 0.0)
        fresh_weights = jnp.where(causal, jnp.exp(fresh - top), 0.0)
        norm = jnp.sum(weights, axis=1, keepdims=True) + jnp.sum(fresh_weights, axis=1, keepdims=True)
        acc = lax.dot_general(
            weights.astype(jnp.bfloat16), k[:latent], (((1,), (1,)), ((), ())), preferred_element_type=jnp.float32
        )
        acc += jnp.dot(fresh_weights.astype(jnp.bfloat16), new[:, :latent], preferred_element_type=jnp.float32)
        live = norm > 0.0
        safe = jnp.where(live, norm, 1.0)
        out_refs[c][0] = (acc / safe).astype(jnp.bfloat16)
        lse = jnp.where(live, top + jnp.log(safe), NEG)
        lse_refs[c][0] = jnp.transpose(jnp.broadcast_to(lse, (rows, 128)))[0:1, :]


def flash(info, start, queries, own_a, own_b, far_a, far_b, new, scale, steps, latent):
    n_ctx = len(queries)
    count = far_a.shape[0]
    rows, width = queries[0].shape[1:]
    half, span = own_a.shape[1:]
    whole = lambda i, s: (start + i, 0, 0)
    chunk = lambda i, s: (i, 0, 0)
    flops = 4 * count * n_ctx * rows * width * 2 * span
    grid_spec = pltpu.PrefetchScalarGridSpec(
        num_scalar_prefetch=1,
        grid=(count,),
        in_specs=[pl.BlockSpec((1, rows, width), whole)]
        + [pl.BlockSpec((1, rows, width), chunk)] * (n_ctx - 1)
        + [pl.BlockSpec((1, half, span), whole)] * 2
        + [pl.BlockSpec((1, half, span), chunk)] * 2
        + [pl.BlockSpec((1,) + new.shape[1:], chunk)],
        out_specs=[pl.BlockSpec((1, rows, latent), chunk)] * n_ctx + [pl.BlockSpec((1, 1, rows), chunk)] * n_ctx,
        scratch_shapes=[pltpu.VMEM((2 * half, 2 * span), jnp.bfloat16)],
    )
    res = pl.pallas_call(
        functools.partial(flash_kernel, scale, steps, latent, n_ctx),
        grid_spec=grid_spec,
        out_shape=[jax.ShapeDtypeStruct((count, rows, latent), jnp.bfloat16)] * n_ctx
        + [jax.ShapeDtypeStruct((count, 1, rows), jnp.float32)] * n_ctx,
        compiler_params=pltpu.CompilerParams(vmem_limit_bytes=24 * 1024 * 1024),
        cost_estimate=pl.CostEstimate(flops=flops, bytes_accessed=count * 4 * half * span * 2, transcendentals=0),
    )(info, *queries, own_a, own_b, far_a, far_b, new)
    return list(res[:n_ctx]), list(res[n_ctx:])


def shards(cache, lengths, request_decode_slot, q_nope, q_rope, new_latent, w_key, value_up_weight):
    total_reqs = request_decode_slot.shape[0]
    n_req = lax.axis_size("req")
    n_ctx = lax.axis_size("ctx")
    req_dev = total_reqs // n_req
    me = lax.axis_index("req")
    ctx = lax.axis_index("ctx")
    role = lax.axis_index("role")
    groups = n_req // 2
    group, side = me // 2, me % 2
    heads, nope, latent = w_key.shape
    steps = q_nope.shape[1]
    rope = q_rope.shape[2] // heads
    vdim = value_up_weight.shape[2]
    span = cache.shape[1]
    scale = (nope + rope) ** (-0.5)
    tie = lax.optimization_barrier

    swap = [(i, i ^ 1) for i in range(n_req)]
    other = [(0, 1), (1, 0)]

    def hop(k):
        return [(i, ((i // 2 - k) % groups) * 2 + i % 2) for i in range(n_req)]

    def turn(k):
        return [(i, (i + k) % n_ctx) for i in range(n_ctx)]

    reach = list(range(1, groups)) + [0]
    slots = jnp.arange(total_reqs, dtype=jnp.int32)
    inverse = jnp.sum(
        jnp.where(request_decode_slot[None, :] == slots[:, None], slots[None, :], 0), axis=1
    ).astype(jnp.int32)
    order = (group + jnp.array(reach, dtype=jnp.int32)) % groups

    def rows_of(which):
        index = (order[:, None] * 2 + which) * req_dev + jnp.arange(req_dev, dtype=jnp.int32)[None, :]
        hit = index[:, :, None] == slots
        return jnp.sum(jnp.where(hit, inverse, 0), axis=2).astype(jnp.int32)

    mine, theirs = rows_of(side), rows_of(1 - side)
    turned = jnp.swapaxes(cache, 1, 2)
    packed = [pack(turned, theirs[n]) for n in range(groups)]
    far_a = [lax.ppermute(x, "req", swap) for x in packed]

    raw = jnp.concatenate([q_nope, q_rope], axis=2)
    raw, _ = tie((raw, packed[0]))
    raws = jnp.stack([raw if k == 0 else lax.ppermute(raw, "req", hop(k)) for k in reach])
    own_a = pack(turned, mine.reshape(-1))
    own_b = lax.ppermute(own_a, "role", other)

    count = groups * req_dev
    raws = raws.reshape(count, steps, -1)
    split = heads * nope
    absorbed = jnp.einsum(
        "bshd,hdk->bshk",
        raws[:, :, :split].reshape(count, steps, heads, nope),
        w_key,
        preferred_element_type=jnp.float32,
    ).astype(jnp.bfloat16)
    queries = jnp.concatenate(
        [absorbed, raws[:, :, split:].reshape(count, steps, heads, rope)], axis=3
    ).reshape(count, steps * heads, latent + rope)
    peers = []
    for n in range(groups):
        part = queries[n * req_dev:(n + 1) * req_dev]
        peers.append([lax.ppermute(part, "ctx", turn(k)) for k in range(1, n_ctx)])

    new = jnp.pad(new_latent, ((0, 0), (0, 128 - steps), (0, 0)))
    base = ctx * n_req * span
    sent_o, sent_l = [None] * groups, [None] * groups

    def finish(n, outs, lses):
        lses = jnp.stack(lses)[:, :, 0, :]
        top = jnp.max(lses, axis=0)
        share = jnp.exp(lses - top[None])
        norm = jnp.sum(share, axis=0)
        share = share / norm[None]
        merged = sum(o.astype(jnp.float32) * share[j][..., None] for j, o in enumerate(outs)).astype(jnp.bfloat16)
        attended = jnp.einsum(
            "poay,ayx->poax",
            merged.reshape(req_dev, steps, heads, latent),
            value_up_weight,
            preferred_element_type=jnp.float32,
        ).astype(jnp.bfloat16).reshape(req_dev, steps, heads * vdim)
        total = top + jnp.log(norm)
        k = reach[n]
        sent_o[n] = attended if k == 0 else lax.ppermute(attended, "req", hop(groups - k))
        sent_l[n] = total if k == 0 else lax.ppermute(total, "req", hop(groups - k))

    last = None
    for n in range(groups):
        fresh_on = ((ctx == 0) & (reach[n] == 0)).astype(jnp.int32)
        info = jnp.concatenate(
            [jnp.stack([role, base + me * span, base + (me ^ 1) * span, fresh_on]), lengths[mine[n]]]
        ).astype(jnp.int32)
        far = far_a[n]
        if last is not None:
            far, last[1][0] = tie((far, last[1][0]))
        far_b = lax.ppermute(far, "role", other)
        outs, lses = flash(
            info, n * req_dev, [queries] + peers[n], own_a, own_b, far, far_b, new, scale, steps, latent
        )
        outs = [outs[0]] + [lax.ppermute(outs[j], "ctx", turn(n_ctx - j)) for j in range(1, n_ctx)]
        if last is not None:
            last[1][0], lses[0] = tie((last[1][0], lses[0]))
            finish(n - 1, last[0], last[1])
        lses = [lses[0]] + [lax.ppermute(lses[j], "ctx", turn(n_ctx - j)) for j in range(1, n_ctx)]
        last = [outs, lses]
    finish(groups - 1, last[0], last[1])

    lses = jnp.stack(sent_l)
    top = jnp.max(lses, axis=0)
    share = jnp.exp(lses - top[None])
    share = (share / jnp.sum(share, axis=0)[None]).reshape(groups, req_dev, steps, heads)
    result = 0.0
    for n in range(groups):
        piece = sent_o[n].reshape(req_dev, steps, heads, vdim).astype(jnp.float32)
        result = result + piece * share[n][..., None]
    return result.astype(jnp.bfloat16).reshape(req_dev, steps, heads * vdim)


def solution(mesh):
    placed = (
        P(None, ("ctx", "req"), "role"),
        P(),
        P(),
        P("req", None, ("role", "ctx")),
        P("req", None, ("role", "ctx")),
        P("req", None, None),
        P(("role", "ctx"), None, None),
        P(("role", "ctx"), None, None),
    )
    return jax.shard_map(
        shards,
        mesh=mesh,
        in_specs=placed,
        out_specs=P("req", None, ("role", "ctx")),
        check_vma=False,
    )
```
